32 devices in a mesh: groups: 1, tensor: 32 (over z, y, x, core).
Axes of the slice: x: 2, y: 2, z: 4, core: 2. Of those that a mesh axis runs over, the one named last changes fastest.
Arguments:
- hidden_in: bfloat16 [4, 16384], P('groups', 'tensor'), may hold values from -0.59765625 to 0.59765625
- norm_gain: bfloat16 [16384], P('tensor'), may hold values from 0.5 to 1.5
- w_q: bfloat16 [16384, 16384], P('tensor'), may hold values from -1 to 256
- w_kv: bfloat16 [16384, 2048], P('tensor'), may hold values from -0.046875 to 0.046875
- w_o: bfloat16 [16384, 16384], P(None, 'tensor'), may hold values from -0.046875 to 0.046875
- kv_cache: bfloat16 [8, 4, 2, 4096, 128], P(None, 'groups', None, 'tensor'), may hold values from -8 to 8
- lengths: int32 [4], P('groups'), may hold values from 2 to 4096, as said below
- slab_index: int32 [8, 4], P(None, 'groups'), may hold values from 0 to 3, each once within a row
Outputs:
- hidden_out: bfloat16 [4, 16384], P('groups', 'tensor')
The draws below stay inside these ranges and needn't reach their ends.
Inputs may be any that keep to these rules, and one draw needn't show every extreme that they name: `lengths`: one request in every draw has exactly 4096 cached tokens.
All inputs are finite; a program needn't handle non-finite values.
Results may differ from the reference program's by a relative error of at most 0.0085.
The reference program's roundings to bfloat16 on the way count: a program that leaves them out, or rounds other values in their place, can miss the bound.
Values may be sent and summed in bfloat16 or wider, within the bound.
A program may use at most 128 MiB of HBM per device.

```python
import jax
import jax.numpy as jnp
from jax import lax

KVH = 8
HD = 128
GROUP = 16
D = 16384
CTX = 4096
BATCH = 4


def draw_lengths(key, part):
    picked = jax.random.randint(jax.random.fold_in(key, 11), (BATCH,), 2, CTX + 1)
    longest = jax.random.randint(jax.random.fold_in(key, 12), (), 0, BATCH)
    return jnp.where(jnp.arange(BATCH) == longest, CTX, picked).astype(jnp.int32)


def draw_w_q(key, part):
    weight_scale = D ** (-0.5)
    base = jax.random.normal(jax.random.fold_in(key, 31), (D, D), jnp.float32) * weight_scale
    base = jnp.clip(base, -6.0 * weight_scale, 6.0 * weight_scale)
    return base.astype(jnp.bfloat16)


def draw_kv_cache(key, part):
    base = 2.0 * jax.random.normal(jax.random.fold_in(key, 21), (KVH, BATCH, 2, CTX, HD), jnp.float32)
    return jnp.clip(base, -8.0, 8.0).astype(jnp.bfloat16)


def block_levels(rng, dims, shards, smallest, largest):
    level = 1.0
    for axis_at, blocks in shards:
        heights = jax.random.uniform(jax.random.fold_in(jax.random.fold_in(rng, 6), axis_at), (blocks,), jnp.float32, smallest / len(shards), largest / len(shards))
        level = level * jnp.repeat(jnp.exp(heights), dims[axis_at] // blocks).reshape((-1,) + (1,) * (len(dims) - 1 - axis_at))
    return level


def noise(rng, dims, width, reach, pieces=(), held_as=jnp.bfloat16):
    gain = block_levels(rng, dims, pieces, -0.22, 0.18) if pieces else 1.0
    values = jax.random.normal(rng, dims, jnp.float32) * width * gain
    return jnp.minimum(jnp.maximum(values, -reach), reach).astype(held_as)


def setup_inputs(seed: int = 0, part: int = 0) -> dict:
    key_of = jax.random.split(jax.random.key(seed), 9)
    own_keys = jax.random.split(jax.random.fold_in(key_of[8], part), 9)
    return {
        "hidden_in": noise(own_keys[0], (BATCH, D), 0.1, 0.59765625, ((1, 32),)),
        "norm_gain": jnp.clip(1.0 + 0.1 * jax.random.normal(key_of[1], (D,), jnp.float32), 0.5, 1.5).astype(jnp.bfloat16),
        "w_q": draw_w_q(jax.random.fold_in(key_of[8], 71), part),
        "w_kv": noise(key_of[3], (D, 2 * KVH * HD), D ** -0.5, 0.046875, ((0, 32),)),
        "w_o": noise(key_of[4], (D, D), D ** -0.5, 0.046875, ((1, 32),)),
        "kv_cache": draw_kv_cache(jax.random.fold_in(jax.random.fold_in(key_of[8], part), 71), part),
        "lengths": draw_lengths(jax.random.fold_in(jax.random.fold_in(key_of[8], part), 71), part),
        "slab_index": jax.vmap(lambda own: jax.random.permutation(own, BATCH))(jax.random.split(own_keys[7], KVH)).reshape((KVH, BATCH)).astype(jnp.int32),
    }


epsilon = 1e-05
rope_base = 500000.0

def rotate(values, position):
    head_dim = values.shape[-1]
    half_dim = head_dim // 2
    frequency = rope_base ** (-2.0 * jnp.arange(half_dim, dtype=jnp.float32) / head_dim)
    angles = position[..., None] * frequency
    cosine = jnp.cos(angles)
    sines = jnp.sin(angles)
    lower_half = values[..., :half_dim]
    upper_half = values[..., half_dim:]
    return jnp.concatenate([lower_half * cosine - upper_half * sines, upper_half * cosine + lower_half * sines], axis=-1)

def reference(hidden_in, norm_gain, w_q, w_kv, w_o, kv_cache, lengths, slab_index):
    stream = hidden_in.astype(jnp.float32)
    squares = lax.optimization_barrier(jnp.mean(stream * stream, axis=1, keepdims=True))
    normed = (stream * lax.rsqrt(squares + epsilon) * norm_gain.astype(jnp.float32)).astype(jnp.bfloat16)
    proj_q = jnp.dot(normed, w_q, preferred_element_type=jnp.float32)
    proj_kv = jnp.dot(normed, w_kv, preferred_element_type=jnp.float32)
    position = lengths.astype(jnp.float32)
    queries = rotate(proj_q.reshape(BATCH, KVH, GROUP, HD), position[:, None, None]).astype(jnp.bfloat16)
    kv_parts = proj_kv.reshape(BATCH, 2, KVH, HD)
    new_keys = rotate(kv_parts[:, 0], position[:, None]).astype(jnp.bfloat16)
    new_values = kv_parts[:, 1].astype(jnp.bfloat16)
    visible = jnp.arange(CTX, dtype=jnp.int32)[None, :] < lengths[:, None]
    score_scale = 1.0 / HD ** 0.5

    def attend_head(kv_head):
        cache_head = kv_cache[kv_head][slab_index[kv_head]]
        key_cache = cache_head[:, 0].astype(jnp.float32)
        value_cache = cache_head[:, 1].astype(jnp.float32)
        head_queries = queries[:, kv_head].astype(jnp.float32)
        scores = jnp.einsum('bgd,bpd->bgp', head_queries, key_cache) * score_scale
        new_score = jnp.einsum('bgd,bd->bg', head_queries, new_keys[:, kv_head].astype(jnp.float32)) * score_scale
        row_max = jnp.maximum(lax.optimization_barrier(jnp.max(jnp.where(visible[:, None, :], scores, -1e+30), axis=2)), new_score)
        weights = jnp.where(visible[:, None, :], jnp.exp(scores - row_max[..., None]), 0.0)
        new_weight = jnp.exp(new_score - row_max)
        denominator = lax.optimization_barrier(jnp.sum(weights, axis=2)) + new_weight
        weighted = jnp.einsum('bgp,bpd->bgd', weights.astype(jnp.bfloat16).astype(jnp.float32), value_cache)
        weighted = weighted + new_weight.astype(jnp.bfloat16).astype(jnp.float32)[..., None] * new_values[:, kv_head].astype(jnp.float32)[:, None, :]
        return (weighted / denominator[..., None]).astype(jnp.bfloat16)
    heads_out = lax.map(attend_head, jnp.arange(KVH, dtype=jnp.int32))
    attention = jnp.transpose(heads_out, (1, 0, 2, 3)).reshape(BATCH, D)
    result = stream + jnp.dot(attention, w_o, preferred_element_type=jnp.float32)
    return result.astype(jnp.bfloat16)
```

```python
import functools

import jax
import jax.numpy as jnp
import numpy as np
from jax import lax
from jax.experimental import pallas as pl
from jax.experimental.pallas import tpu as pltpu
from jax.sharding import PartitionSpec as P

KVH = 8
HD = 128
GROUP = 16

epsilon = 1e-05
rope_base = 500000.0
score_scale = 1.0 / HD**0.5
lowest = -1e30
STAGES = 4


def step_kernel(
    n,
    slab_hbm,
    len_hbm,
    hidden_hbm,
    gain_hbm,
    freq_hbm,
    wq_hbm,
    wkv_hbm,
    wo_hbm,
    kv_hbm,
    out_ref,
    slab_ref,
    len_ref,
    hidden_v,
    gain_v,
    freq_v,
    wq_v,
    wkv_v,
    wo_v,
    kv_v,
    sq_buf,
    kvp,
    kv_d,
    kv_sum,
    kv_in,
    kv_sib,
    kv_flat,
    q_other,
    q_own,
    q_d,
    q_in,
    q_buf,
    k_rows,
    v_rows,
    o_buf,
    o_in,
    st_buf,
    st_in,
    att_f,
    att_buf,
    small_sem,
    wq_sem,
    wkv_sem,
    wo_sem,
    kv_sem,
    send_sem,
    recv_sem,
    pair_sem,
    att_sem,
):
    me = lax.axis_index("tensor")
    requests, width = hidden_hbm.shape
    chips = n // 2
    chip, core = me // 2, lax.rem(me, 2)
    partner = chip * 2 + 1 - core
    heads = KVH * GROUP // n
    cols = heads * HD
    q_rows = heads * requests
    per_kv = GROUP // heads
    half_kv = KVH // 2
    kv_rows = 2 * requests // per_kv
    slabs, positions = kv_hbm.shape[1], kv_hbm.shape[3]
    span = 2 * positions
    in_stage = chips // STAGES

    flips = []
    bit = 1
    while bit < n:
        flips.append(bit * (1 - 2 * lax.rem(me // bit, 2)))
        bit *= 2

    def flipped(mask):
        peer = me
        for k, flip in enumerate(flips):
            if mask >> k & 1:
                peer = peer + flip
        return peer

    def block_of(device):
        return lax.rem(device, 2) * chips + device // 2

    far_first = list(range(n - 1, 0, -1))
    chip_order = list(range(chips - 1, -1, -1))

    barrier = pltpu.get_barrier_semaphore()
    for mask in far_first:
        pl.semaphore_signal(
            barrier,
            inc=1,
            device_id={"tensor": flipped(mask)},
            device_id_type=pl.DeviceIdType.MESH,
        )

    small = [
        pltpu.make_async_copy(src, dst, small_sem.at[k])
        for k, (src, dst) in enumerate(
            (
                (hidden_hbm, hidden_v),
                (gain_hbm, gain_v),
                (len_hbm, len_ref),
                (freq_hbm, freq_v),
                (slab_hbm, slab_ref),
            )
        )
    ]
    for copy in small:
        copy.start()

    def wq_copy(block, slot):
        return pltpu.make_async_copy(
            wq_hbm.at[:, pl.ds(pl.multiple_of(block * cols, cols), cols)],
            wq_v.at[slot],
            wq_sem.at[slot],
        )

    wkv_copy = pltpu.make_async_copy(wkv_hbm, wkv_v, wkv_sem)
    wo_copy = pltpu.make_async_copy(wo_hbm, wo_v, wo_sem)
    wkv_copy.start()
    wq_copies = []
    for step, mask in enumerate(chip_order):
        device = flipped(2 * mask)
        target = device // 2
        wq_copies.append(wq_copy((1 - core) * chips + target, 2 * step))
        wq_copies.append(wq_copy(core * chips + target, 2 * step + 1))
    for copy in wq_copies:
        copy.start()

    def remote(src, dst, sent, received, peer):
        return pltpu.make_async_remote_copy(
            src_ref=src,
            dst_ref=dst,
            send_sem=sent,
            recv_sem=received,
            device_id={"tensor": peer},
            device_id_type=pl.DeviceIdType.MESH,
        )

    def every(buf, phase, count):
        part = buf.at[pl.ds(0, count)]
        return remote(part, part, send_sem.at[phase], recv_sem.at[phase], partner)

    small[0].wait()
    stream = hidden_v[...].astype(jnp.float32)
    own_sq = jnp.sum(stream * stream, axis=1, keepdims=True)
    sq_row = lax.broadcasted_iota(jnp.int32, (requests, HD), 0)
    sq_lane = lax.broadcasted_iota(jnp.int32, (requests, HD), 1)
    sq_diagonal = sq_row == sq_lane
    sq_buf[me] = jnp.sum(jnp.where(sq_diagonal, own_sq, 0.0), axis=0, keepdims=True)

    pl.semaphore_wait(barrier, n - 1)
    for mask in far_first:
        remote(
            sq_buf.at[me], sq_buf.at[me], send_sem.at[0], recv_sem.at[0], flipped(mask)
        ).start()

    own_place = pl.ds(pl.multiple_of(core * positions, positions), positions)
    kv_copy = pltpu.make_async_copy(
        kv_hbm.at[pl.ds(core * half_kv, half_kv)], kv_v.at[:, :, :, own_place], kv_sem.at[0]
    )
    kv_swap = remote(
        kv_hbm.at[pl.ds((1 - core) * half_kv, half_kv)],
        kv_v.at[:, :, :, own_place],
        kv_sem.at[1],
        kv_sem.at[2],
        partner,
    )
    kv_copy.start()
    kv_swap.start()

    for copy in small[1:]:
        copy.wait()
    gain = jnp.concatenate(
        [gain_v[k : k + 1, :].astype(jnp.float32) for k in range(width // HD)], axis=1
    )

    def tables(rows, first):
        row = lax.broadcasted_iota(jnp.int32, (rows, HD), 0) + first
        lane = lax.broadcasted_iota(jnp.int32, (rows, HD), 1)
        request = lax.rem(row, requests)
        length = jnp.zeros((rows, HD), jnp.float32)
        for b in range(requests):
            length = jnp.where(request == b, len_ref[b].astype(jnp.float32), length)
        angles = length * freq_v[...]
        sine = jnp.sin(angles)
        return row, jnp.cos(angles), jnp.where(lane < HD // 2, -sine, sine)

    member = lax.rem(chip, per_kv)
    _, q_cos, q_sin = tables(q_rows, 0)
    kv_row, kv_cos, kv_sin = tables(kv_rows, member * kv_rows)
    kv_cos = jnp.where(kv_row < requests, kv_cos, 1.0)
    kv_sin = jnp.where(kv_row < requests, kv_sin, 0.0)

    wkv_copy.wait()
    for copy in wq_copies:
        copy.wait()
    every(sq_buf, 0, n - 1).wait_recv()
    sq_total = jnp.sum(sq_buf[...], axis=0)
    squares = jnp.sum(jnp.where(sq_diagonal, sq_total, 0.0), axis=1, keepdims=True)
    normed = (stream * lax.rsqrt(squares / (width * n) + epsilon) * gain).astype(jnp.bfloat16)

    proj_kv = jnp.dot(normed, wkv_v[...], preferred_element_type=jnp.float32)
    for head in range(KVH):
        for t in range(per_kv):
            part, first = divmod(t * kv_rows, requests)
            lanes = (part * KVH + head) * HD
            kvp[head * per_kv + t] = proj_kv[first : first + kv_rows, lanes : lanes + HD]
    kv_pair = remote(
        kvp.at[pl.ds((1 - core) * chips, chips)],
        kv_d,
        pair_sem.at[0, STAGES],
        pair_sem.at[1, STAGES],
        partner,
    )
    kv_pair.start()

    def stage_slots(stage):
        return pl.ds(stage * in_stage, in_stage)

    def pair_copy(stage):
        return remote(
            q_other.at[stage_slots(stage)],
            q_d.at[stage_slots(stage)],
            pair_sem.at[0, stage],
            pair_sem.at[1, stage],
            partner,
        )

    def project(stage):
        for target, side in ((q_other, 0), (q_own, 1)):
            for step in range(stage * in_stage, (stage + 1) * in_stage):
                res = jnp.dot(normed, wq_v[2 * step + side], preferred_element_type=jnp.float32)
                for j in range(heads):
                    target[step, j * requests : (j + 1) * requests, :] = res[
                        :, j * HD : (j + 1) * HD
                    ]
        pair_copy(stage).start()

    def forward(stage):
        if stage == 0:
            kv_pair.wait_recv()
            kv_sum[...] = kvp[pl.ds(core * chips, chips)] + kv_d[...]
        pair_copy(stage).wait_recv()
        slots = slice(stage * in_stage, (stage + 1) * in_stage)
        q_own[slots] = q_own[slots] + q_d[slots]
        for step in range(stage * in_stage, (stage + 1) * in_stage):
            mask = chip_order[step]
            if mask:
                peer = flipped(2 * mask)
                remote(
                    q_own.at[step], q_in.at[chip], send_sem.at[1], recv_sem.at[1], peer
                ).start()
                remote(
                    kv_sum.at[peer // 2], kv_in.at[chip], send_sem.at[2], recv_sem.at[2], peer
                ).start()
            else:
                q_in[chip] = q_own[step]
                kv_in[chip] = kv_sum[chip]

    for stage in range(STAGES):
        project(stage)
        if stage >= 2:
            forward(stage - 2)
    forward(STAGES - 2)
    forward(STAGES - 1)
    wo_copy.start()

    every(q_in, 1, chips - 1).wait_recv()
    total = jnp.sum(q_in[...], axis=0)
    total = total * q_cos + pltpu.roll(total, HD // 2, 1) * q_sin
    rounded = total.astype(jnp.bfloat16)
    queries_own = rounded.astype(jnp.float32)
    q_buf[chip] = rounded
    for mask in chip_order[:-1]:
        remote(
            q_buf.at[chip], q_buf.at[chip], send_sem.at[3], recv_sem.at[3], flipped(2 * mask)
        ).start()

    every(kv_in, 2, chips - 1).wait_recv()
    kv_total = jnp.sum(kv_in[...], axis=0)
    kv_total = kv_total * kv_cos + pltpu.roll(kv_total, HD // 2, 1) * kv_sin
    kv_sib[member] = kv_total.astype(jnp.bfloat16).astype(jnp.float32)
    for step in range(1, per_kv):
        sibling = chip - member + lax.rem(member + step, per_kv)
        remote(
            kv_sib.at[member],
            kv_sib.at[member],
            send_sem.at[4],
            recv_sem.at[4],
            sibling * 2 + core,
        ).start()
    every(kv_sib, 4, per_kv - 1).wait_recv()
    for t in range(per_kv):
        kv_flat[t * kv_rows : (t + 1) * kv_rows, :] = kv_sib[t]
    for j in range(heads):
        k_rows[j * requests : (j + 1) * requests, :] = kv_flat[:requests, :]
        v_rows[j * requests : (j + 1) * requests, :] = kv_flat[requests:, :]
    new_score = jnp.sum(queries_own * k_rows[...], axis=1, keepdims=True) * score_scale
    lane = lax.broadcasted_iota(jnp.int32, (q_rows, HD), 1)
    row = lax.broadcasted_iota(jnp.int32, (q_rows, HD), 0)
    diagonal = lane == row
    shifted = lane == row + HD // 2
    new_lane = jnp.sum(jnp.where(diagonal, new_score, 0.0), axis=0, keepdims=True)

    all_rows = GROUP * requests
    row_req = lax.rem(lax.broadcasted_iota(jnp.int32, (all_rows, 1), 0), requests)
    column_pos = lax.broadcasted_iota(jnp.int32, (1, span), 1) + chip * span
    row_len = jnp.zeros((all_rows, 1), jnp.int32)
    for b in range(requests):
        row_len = jnp.where(row_req == b, len_ref[b], row_len)
    visible = column_pos < row_len

    kv_copy.wait()
    kv_swap.wait_recv()
    every(q_buf, 3, chips - 1).wait_recv()

    for h in range(half_kv):
        queries = q_buf[h * per_kv : (h + 1) * per_kv].reshape(all_rows, HD)
        places = [slab_ref[b, core * half_kv + h] for b in range(requests)]
        scores = None
        for b in range(requests):
            part = lax.dot_general(
                queries,
                kv_v[h, places[b], 0],
                (((1,), (1,)), ((), ())),
                preferred_element_type=jnp.float32,
            )
            scores = part if b == 0 else jnp.where(row_req == b, part, scores)
        scores = jnp.where(visible, scores * score_scale, lowest)
        top = jnp.max(scores, axis=1, keepdims=True)
        weights = jnp.where(visible, jnp.exp(scores - top), 0.0)
        weight_sum = jnp.sum(weights, axis=1, keepdims=True)
        weighted = jnp.zeros((all_rows, HD), jnp.float32)
        for b in range(requests):
            weighted = weighted + jnp.dot(
                jnp.where(row_req == b, weights, 0.0).astype(jnp.bfloat16),
                kv_v[h, places[b], 1],
                preferred_element_type=jnp.float32,
            )
        for t in range(per_kv):
            own = slice(t * q_rows, (t + 1) * q_rows)
            o_buf[h * per_kv + t] = weighted[own].astype(jnp.bfloat16)
            st_buf[h * per_kv + t] = jnp.sum(
                jnp.where(diagonal, top[own], 0.0) + jnp.where(shifted, weight_sum[own], 0.0),
                axis=0,
                keepdims=True,
            )

    for mask in chip_order[:-1]:
        peer = flipped(2 * mask)
        remote(
            st_buf.at[peer // 2], st_in.at[chip], send_sem.at[5], recv_sem.at[5], peer
        ).start()
        remote(o_buf.at[peer // 2], o_in.at[chip], send_sem.at[6], recv_sem.at[6], peer).start()
    o_in[chip] = o_buf[chip]
    st_in[chip] = st_buf[chip]

    every(st_in, 5, chips - 1).wait_recv()
    stats = st_in[...]
    top_lane = jnp.maximum(jnp.max(stats, axis=0), new_lane)
    factor = jnp.exp(jnp.minimum(stats - top_lane[None], 0.0))
    new_factor = jnp.exp(new_lane - top_lane)
    sums = jnp.concatenate([stats[:, :, HD // 2 :], stats[:, :, : HD // 2]], axis=2)
    denominator_lane = jnp.sum(factor * sums, axis=0) + new_factor

    def as_column(lanes):
        return jnp.sum(jnp.where(diagonal, lanes, 0.0), axis=1, keepdims=True)

    weighted = as_column(new_factor).astype(jnp.bfloat16).astype(jnp.float32) * v_rows[...]
    columns = jnp.sum(jnp.where(diagonal[None], factor, 0.0), axis=2, keepdims=True)
    denominator = as_column(denominator_lane)
    every(o_in, 6, chips - 1).wait_recv()
    weighted = weighted + jnp.sum(columns * o_in[...].astype(jnp.float32), axis=0)
    att_f[...] = weighted / denominator
    for j in range(heads):
        att_buf[me, :, j * HD : (j + 1) * HD] = att_f[
            j * requests : (j + 1) * requests, :
        ].astype(jnp.bfloat16)

    groups = [list(range(first, first + n // 4)) for first in range(0, n, n // 4)]
    group_of = {mask: k for k, group in enumerate(groups) for mask in group}
    for mask in far_first:
        remote(
            att_buf.at[me],
            att_buf.at[me],
            send_sem.at[7],
            att_sem.at[group_of[mask]],
            flipped(mask),
        ).start()

    wo_copy.wait()
    acc = stream
    for k, group in enumerate(groups):
        count = sum(mask > 0 for mask in group)
        part = att_buf.at[pl.ds(0, count)]
        remote(part, part, send_sem.at[7], att_sem.at[k], partner).wait_recv()
        for mask in group:
            source = flipped(mask)
            first = pl.multiple_of(block_of(source) * cols, cols)
            acc = acc + jnp.dot(
                att_buf[source],
                wo_v[pl.ds(first, cols), :],
                preferred_element_type=jnp.float32,
            )
    out_ref[...] = acc.astype(jnp.bfloat16)

    kv_swap.wait_send()
    kv_pair.wait_send()
    for stage in range(STAGES):
        pair_copy(stage).wait_send()
    every(sq_buf, 0, n - 1).wait_send()
    every(q_in, 1, chips - 1).wait_send()
    every(kv_in, 2, chips - 1).wait_send()
    every(q_buf, 3, chips - 1).wait_send()
    every(kv_sib, 4, per_kv - 1).wait_send()
    every(st_in, 5, chips - 1).wait_send()
    every(o_in, 6, chips - 1).wait_send()
    every(att_buf, 7, n - 1).wait_send()


def body(n, hidden_in, norm_gain, w_q, w_kv, w_o, kv_cache, lengths, slab_index):
    requests, width = hidden_in.shape
    chips = n // 2
    heads = KVH * GROUP // n
    cols = heads * HD
    q_rows = heads * requests
    per_kv = GROUP // heads
    kv_rows = 2 * requests // per_kv
    slabs, positions = kv_cache.shape[1], kv_cache.shape[3]

    exponent = -2.0 * (np.arange(HD) % (HD // 2)) / HD
    frequency = jnp.asarray((rope_base**exponent).astype(np.float32).reshape(1, HD))

    hbm = pl.BlockSpec(memory_space=pltpu.HBM)
    bf16, f32 = jnp.bfloat16, jnp.float32
    dma = pltpu.SemaphoreType.DMA
    return pl.pallas_call(
        functools.partial(step_kernel, n),
        out_shape=jax.ShapeDtypeStruct((requests, width), bf16),
        in_specs=[hbm] * 9,
        out_specs=pl.BlockSpec(memory_space=pltpu.VMEM),
        scratch_shapes=[
            pltpu.SMEM((requests, KVH), jnp.int32),
            pltpu.SMEM((requests,), jnp.int32),
            pltpu.VMEM((requests, width), bf16),
            pltpu.VMEM((width // HD, HD), bf16),
            pltpu.VMEM((1, HD), f32),
            pltpu.VMEM((n, width, cols), bf16),
            pltpu.VMEM(w_kv.shape, bf16),
            pltpu.VMEM(w_o.shape, bf16),
            pltpu.VMEM((KVH // 2, slabs, 2, 2 * positions, HD), bf16),
            pltpu.VMEM((n, 1, HD), f32),
            pltpu.VMEM((n, kv_rows, HD), f32),
            pltpu.VMEM((chips, kv_rows, HD), f32),
            pltpu.VMEM((chips, kv_rows, HD), f32),
            pltpu.VMEM((chips, kv_rows, HD), f32),
            pltpu.VMEM((per_kv, kv_rows, HD), f32),
            pltpu.VMEM((2 * requests, HD), f32),
            pltpu.VMEM((chips, q_rows, HD), f32),
            pltpu.VMEM((chips, q_rows, HD), f32),
            pltpu.VMEM((chips, q_rows, HD), f32),
            pltpu.VMEM((chips, q_rows, HD), f32),
            pltpu.VMEM((chips, q_rows, HD), bf16),
            pltpu.VMEM((q_rows, HD), f32),
            pltpu.VMEM((q_rows, HD), f32),
            pltpu.VMEM((chips, q_rows, HD), bf16),
            pltpu.VMEM((chips, q_rows, HD), bf16),
            pltpu.VMEM((chips, 1, HD), f32),
            pltpu.VMEM((chips, 1, HD), f32),
            pltpu.VMEM((q_rows, HD), f32),
            pltpu.VMEM((n, requests, cols), bf16),
            dma((5,)),
            dma((n,)),
            dma,
            dma,
            dma((3,)),
            dma((8,)),
            dma((7,)),
            dma((2, STAGES + 1)),
            dma((4,)),
        ],
        compiler_params=pltpu.CompilerParams(
            collective_id=0, has_side_effects=True, vmem_limit_bytes=44 * 1024 * 1024
        ),
    )(
        *(
            pltpu.with_memory_space_constraint(operand, pltpu.HBM)
            for operand in (
                slab_index.T,
                lengths,
                hidden_in,
                norm_gain.reshape(width // HD, HD),
                frequency,
                w_q,
                w_kv,
                w_o,
                kv_cache,
            )
        )
    )


def solution(mesh):
    placed = (
        P("groups", "tensor"),
        P("tensor"),
        P("tensor", None),
        P("tensor", None),
        P(None, "tensor"),
        P(None, "groups", None, "tensor", None),
        P("groups"),
        P(None, "groups"),
    )
    return jax.shard_map(
        functools.partial(body, mesh.shape["tensor"]),
        mesh=mesh,
        in_specs=placed,
        out_specs=P("groups", "tensor"),
        check_vma=False,
    )
```
